32 devices in a mesh: dp: 4 (over y, z), fsdp: 8 (over x, core).
Axes of the slice: x: 4, y: 2, z: 2, core: 2. Of those that a mesh axis runs over, the one named last changes fastest.
The devices are a block of a 4x4x8 slice.
Arguments:
- tokens: bfloat16 [512, 128, 2560], P(('dp', 'fsdp')), parts along dimension 0
- gain_in: bfloat16 [2560], P('fsdp')
- w_dq: bfloat16 [2560, 768], P('fsdp')
- gain_q: bfloat16 [768], P('fsdp')
- w_uq: bfloat16 [768, 3840], P('fsdp')
- w_dkv: bfloat16 [2560, 288], P('fsdp')
- gain_kv: bfloat16 [256], P('fsdp')
- w_ukv: bfloat16 [256, 5120], P('fsdp')
- w_out: bfloat16 [2560, 2560], P('fsdp')
Outputs:
- output 1: bfloat16 [512, 128, 2560], P(('dp', 'fsdp')), parts along dimension 0
- output 2: bfloat16 [512, 128, 256], P(('dp', 'fsdp')), parts along dimension 0
- output 3: bfloat16 [512, 128, 32], P(('dp', 'fsdp')), parts along dimension 0
There are 4 independent parts. The reference program is written for one: setup_inputs(seed, part) draws one part's arguments, and reference() takes and returns one part's arrays. A program takes and returns all parts, laid end to end along the dimension named above; an argument that names none is the same for every part.
All inputs are finite; a program needn't handle non-finite values.
Results may differ from the reference program's by a relative error of at most 0.00648171.
Values are sent between devices in bfloat16 or wider.
A program may use at most 768 MiB of HBM per device.

```python
import jax
import jax.numpy as jnp
from jax import lax

PROMPTS = 128
SEQ_LEN = 128
D_MODEL = 2560
N_HEADS = 40
Q_RANK = 768
KV_RANK = 256
NOPE_DIM = 64
ROPE_DIM = 32
V_DIM = 64
EPSILON = 1e-6
ROPE_THETA = 10000.0


def setup_inputs(seed: int = 0, part: int = 0) -> dict:
    key_list = jax.random.split(jax.random.key(seed), 9)

    def draw_weight(sub_key, n_rows, n_cols):
        drawn = jax.random.normal(sub_key, (n_rows, n_cols), jnp.float32) * (n_rows ** -0.5)
        return drawn.astype(jnp.bfloat16)

    def draw_gain(sub_key, n_items, centre):
        drawn = centre * (1.0 + 0.3 * jax.random.normal(sub_key, (n_items,), jnp.float32))
        return drawn.astype(jnp.bfloat16)

    tok_key = jax.random.fold_in(key_list[0], part)
    tokens = jax.random.normal(tok_key, (PROMPTS, SEQ_LEN, D_MODEL), jnp.float32).astype(jnp.bfloat16)
    return {
        'tokens': tokens,
        'gain_in': draw_gain(key_list[1], D_MODEL, 1.0),
        'w_dq': draw_weight(key_list[2], D_MODEL, Q_RANK),
        'gain_q': draw_gain(key_list[3], Q_RANK, 2.0),
        'w_uq': draw_weight(key_list[4], Q_RANK, N_HEADS * (NOPE_DIM + ROPE_DIM)),
        'w_dkv': draw_weight(key_list[5], D_MODEL, KV_RANK + ROPE_DIM),
        'gain_kv': draw_gain(key_list[6], KV_RANK, 1.0),
        'w_ukv': draw_weight(key_list[7], KV_RANK, N_HEADS * (NOPE_DIM + V_DIM)),
        'w_out': draw_weight(key_list[8], N_HEADS * V_DIM, D_MODEL),
    }


def rms_scale(values_in, gain_vec):
    values_f32 = values_in.astype(jnp.float32)
    inv_rms = lax.rsqrt(jnp.mean(values_f32 * values_f32, axis=-1, keepdims=True) + EPSILON)
    return values_f32 * inv_rms * gain_vec.astype(jnp.float32)


def rope_tables():
    half_dim = ROPE_DIM // 2
    inv_freq = ROPE_THETA ** (-2.0 * jnp.arange(half_dim, dtype=jnp.float32) / ROPE_DIM)
    angles = jnp.arange(SEQ_LEN, dtype=jnp.float32)[:, None] * inv_freq[None, :]
    return jnp.cos(angles), jnp.sin(angles)


def apply_rope(values_in, cos_t, sin_t):
    half_dim = values_in.shape[-1] // 2
    lo_half = values_in[..., :half_dim]
    hi_half = values_in[..., half_dim:]
    return jnp.concatenate([lo_half * cos_t - hi_half * sin_t, hi_half * cos_t + lo_half * sin_t], axis=-1)


def one_prompt(tok_rows, gain_in, w_dq, gain_q, w_uq, w_dkv, gain_kv, w_ukv, w_out):
    cos_t, sin_t = rope_tables()
    normed = rms_scale(tok_rows, gain_in).astype(jnp.bfloat16)
    q_down = jnp.dot(normed, w_dq, preferred_element_type=jnp.float32)
    q_lat = rms_scale(q_down, gain_q).astype(jnp.bfloat16)
    q_full = jnp.dot(q_lat, w_uq, preferred_element_type=jnp.float32).reshape(SEQ_LEN, N_HEADS, NOPE_DIM + ROPE_DIM)
    q_nope = q_full[:, :, :NOPE_DIM].astype(jnp.bfloat16)
    q_pe = apply_rope(q_full[:, :, NOPE_DIM:], cos_t[:, None, :], sin_t[:, None, :]).astype(jnp.bfloat16)
    kv_down = jnp.dot(normed, w_dkv, preferred_element_type=jnp.float32)
    latent = rms_scale(kv_down[:, :KV_RANK], gain_kv).astype(jnp.bfloat16)
    k_pe = apply_rope(kv_down[:, KV_RANK:], cos_t, sin_t).astype(jnp.bfloat16)
    kv_up = jnp.dot(latent, w_ukv, preferred_element_type=jnp.float32).astype(jnp.bfloat16)
    kv_up = kv_up.reshape(SEQ_LEN, N_HEADS, NOPE_DIM + V_DIM)
    k_nope = kv_up[:, :, :NOPE_DIM].astype(jnp.float32)
    values = kv_up[:, :, NOPE_DIM:].astype(jnp.float32)
    score_scale = (NOPE_DIM + ROPE_DIM) ** -0.5
    scores = jnp.einsum('qhd,khd->hqk', q_nope.astype(jnp.float32), k_nope)
    scores = scores + jnp.einsum('qhd,kd->hqk', q_pe.astype(jnp.float32), k_pe.astype(jnp.float32))
    causal = jnp.arange(SEQ_LEN)[:, None] >= jnp.arange(SEQ_LEN)[None, :]
    scores = jnp.where(causal[None, :, :], scores * score_scale, -1e30)
    attn_probs = jax.nn.softmax(scores, axis=-1).astype(jnp.bfloat16)
    attn_out = jnp.einsum('hqk,khd->qhd', attn_probs.astype(jnp.float32), values).astype(jnp.bfloat16)
    attn_out = attn_out.reshape(SEQ_LEN, N_HEADS * V_DIM)
    proj_out = jnp.dot(attn_out, w_out, preferred_element_type=jnp.float32)
    y_rows = (tok_rows.astype(jnp.float32) + proj_out).astype(jnp.bfloat16)
    return y_rows, latent, k_pe


def reference(tokens, gain_in, w_dq, gain_q, w_uq, w_dkv, gain_kv, w_ukv, w_out):
    def per_prompt(tok_rows):
        return one_prompt(tok_rows, gain_in, w_dq, gain_q, w_uq, w_dkv, gain_kv, w_ukv, w_out)

    y_out, kv_cache, pe_cache = lax.map(per_prompt, tokens)
    return (y_out, kv_cache, pe_cache)
```

```python
import functools
import math

import jax
import jax.numpy as jnp
from jax import lax
from jax.experimental import pallas as pl
from jax.experimental.pallas import tpu as pltpu
from jax.sharding import PartitionSpec as P

EPSILON = 1e-6
ROPE_THETA = 10000.0
BF16 = jnp.bfloat16
F32 = jnp.float32
MESH = pl.DeviceIdType.MESH

SPLIT = {320: (112, 96), 96: (32, 32), 32: (16, 0)}
N_KINDS = 11
GROUPS = 5
DQ_CUTS = 3
OUT_CUTS = 5
BLOCK = 256


def rope_tables(seq_len, rope_dim):
    half_dim = rope_dim // 2
    inv_freq = ROPE_THETA ** (-2.0 * jnp.arange(half_dim, dtype=F32) / rope_dim)
    angles = jnp.arange(seq_len, dtype=F32)[:, None] * inv_freq[None, :]
    return jnp.cos(angles), jnp.sin(angles)


def nt_dot(lhs, rhs):
    return lax.dot_general(lhs, rhs, (((1,), (1,)), ((), ())), preferred_element_type=F32)


class Piece:
    def __init__(self, base, src, dst, rows):
        self.base, self.src, self.dst, self.rows = base, src, dst, rows
        self.m, self.c = SPLIT[rows]


def gather_kernel(dims, x_hbm, gains_hbm, dq_hbm, uq_hbm, dkv_hbm, ukv_hbm, out_hbm,
                  cos_r, sin_lo, sin_hi, cos_t, sin_t,
                  o_hbm, lat_hbm, pe_hbm, wout_hbm,
                  gains_all, w_dkv, w_dq, w_uq, w_ukv, w_out,
                  a_buf, qd_buf, cq_buf, lat_buf, pe_buf, rcomb, x_buf, wqt, qf, o_blk,
                  send_sem, recv_sem, own_sem, gain_send, gain_recv, x_sem, o_sem, fin_sem):
    n_fsdp, seq_len, kv_rank, rope_dim, nope, v_dim, heads_per_group = dims
    half = rope_dim // 2
    head_q = nope + rope_dim
    n_tok, d_model = a_buf.shape
    n_blk = n_tok // BLOCK
    q_rank = cq_buf.shape[1]
    me = lax.axis_index('fsdp')
    dp = lax.axis_index('dp')
    n_x = n_fsdp // 2
    core = me % 2
    xx = me // 2
    right = ((xx + 1) % n_x) * 2 + core
    left = ((xx + n_x - 1) % n_x) * 2 + core
    far = ((xx + 2) % n_x) * 2 + core
    mate = xx * 2 + 1 - core
    par = dp % 2
    dp_mate = dp + 1 - 2 * par

    barrier = pltpu.get_barrier_semaphore()
    for k in range(1, n_fsdp):
        pl.semaphore_signal(barrier, inc=1, device_id={'fsdp': (me + k) % n_fsdp}, device_id_type=MESH)
    pl.semaphore_signal(barrier, inc=1, device_id={'dp': dp_mate}, device_id_type=MESH)

    def x_copy(blk, slot):
        return pltpu.make_async_copy(x_hbm.at[pl.ds(blk * BLOCK, BLOCK), :], x_buf.at[slot], x_sem.at[slot])

    x_copy(0, 0).start()

    def rows_of(ref, owner, rows, off, count, cols=None):
        start = pl.multiple_of(owner * rows + off, 16)
        return ref.at[pl.ds(start, count), :]

    pieces = {}
    base = [0]

    def add(unit, src, dst, rows):
        pieces.setdefault(unit, []).append(Piece(base[0], src, dst, rows))
        base[0] += 1

    add(0, dkv_hbm, w_dkv, dkv_hbm.shape[0])
    cut = q_rank // DQ_CUTS
    for j in range(DQ_CUTS):
        add(1 + j, dq_hbm.at[:, pl.ds(j * cut, cut)], w_dq.at[j], dq_hbm.shape[0])
    uq_cols, ukv_cols = heads_per_group * head_q, heads_per_group * (nope + v_dim)
    for g in range(GROUPS):
        add(1 + DQ_CUTS + g, uq_hbm.at[:, pl.ds(g * uq_cols, uq_cols)], w_uq.at[g], uq_hbm.shape[0])
        add(1 + DQ_CUTS + g, ukv_hbm.at[:, pl.ds(g * ukv_cols, ukv_cols)], w_ukv.at[g], ukv_hbm.shape[0])
    out_cols = out_hbm.shape[1] // OUT_CUTS
    for j in range(OUT_CUTS):
        add(1 + DQ_CUTS + GROUPS + j, out_hbm.at[:, pl.ds(j * out_cols, out_cols)], w_out.at[j], out_hbm.shape[0])
    n_units = 1 + DQ_CUTS + GROUPS + OUT_CUTS

    def copy(p, kind, owner, off, count, to, from_own=False):
        start = pl.multiple_of(off, 16) if not isinstance(off, int) else off
        dst = rows_of(p.dst, owner, p.rows, off, count)
        src = p.src.at[pl.ds(start, count), :] if from_own else dst
        return pltpu.make_async_remote_copy(
            src_ref=src, dst_ref=dst, send_sem=send_sem.at[p.base, kind], recv_sem=recv_sem.at[p.base, kind],
            device_id=to, device_id_type=MESH)

    def geom(p):
        edge = p.rows - p.m - p.c
        x_off = par * edge
        m_off = par * (p.rows - p.m)
        z_off = (1 - par) * (p.rows - p.m)
        return x_off, m_off, z_off

    to_right, to_left, to_mate, to_dp = {'fsdp': right}, {'fsdp': left}, {'fsdp': mate}, {'dp': dp_mate}
    mate_of = lambda owner: owner + 1 - 2 * core

    def own_copy(p):
        return pltpu.make_async_copy(p.src, rows_of(p.dst, me, p.rows, 0, p.rows), own_sem.at[p.base])

    def start_own(unit):
        for p in pieces[unit]:
            x_off, _, _ = geom(p)
            copy(p, 0, me, x_off, p.m + p.c, to_right, True).start()
            copy(p, 1, me, x_off, p.m + p.c, to_left, True).start()
            copy(p, 7, me, 0, p.rows, to_mate, True).start()
            own_copy(p).start()

    def stage1(unit):
        for p in pieces[unit]:
            x_off, m_off, _ = geom(p)
            copy(p, 0, left, x_off, p.m + p.c, to_right).wait_recv()
            copy(p, 2, left, m_off, p.m, to_right).start()
            copy(p, 4, left, m_off, p.m, to_dp).start()
            copy(p, 1, right, x_off, p.m + p.c, to_left).wait_recv()
            if p.c:
                copy(p, 3, right, p.m, p.c, to_left).start()
            copy(p, 5, right, m_off, p.m, to_dp).start()

    def stage2(unit):
        for p in pieces[unit]:
            _, m_off, _ = geom(p)
            copy(p, 2, far, m_off, p.m, to_right).wait_recv()
            copy(p, 6, far, m_off, p.m, to_dp).start()
            if p.c:
                copy(p, 3, far, p.m, p.c, to_left).wait_recv()

    def stage3(unit):
        for p in pieces[unit]:
            _, _, z_off = geom(p)
            for kind, owner in ((4, left), (5, right), (6, far)):
                copy(p, kind, owner, z_off, p.m, to_dp).wait_recv()
                copy(p, kind + 4, owner, 0, p.rows, to_mate).start()

    def stage4(unit):
        for p in pieces[unit]:
            for kind, owner in ((7, me), (8, left), (9, right), (10, far)):
                copy(p, kind, mate_of(owner), 0, p.rows, to_mate).wait_recv()
            own_copy(p).wait()

    def all_sent(unit):
        for p in pieces[unit]:
            x_off, m_off, _ = geom(p)
            copy(p, 0, me, x_off, p.m + p.c, to_right, True).wait_send()
            copy(p, 1, me, x_off, p.m + p.c, to_left, True).wait_send()
            copy(p, 2, left, m_off, p.m, to_right).wait_send()
            if p.c:
                copy(p, 3, right, p.m, p.c, to_left).wait_send()
            for kind, owner in ((4, left), (5, right), (6, far)):
                copy(p, kind, owner, m_off, p.m, to_dp).wait_send()
            copy(p, 7, me, 0, p.rows, to_mate, True).wait_send()
            for kind, owner in ((8, left), (9, right), (10, far)):
                copy(p, kind, owner, 0, p.rows, to_mate).wait_send()

    pl.semaphore_wait(barrier, n_fsdp)

    def gain_copy(k, owner):
        return pltpu.make_async_remote_copy(
            src_ref=gains_hbm, dst_ref=gains_all.at[owner], send_sem=gain_send.at[k], recv_sem=gain_recv.at[k],
            device_id={'fsdp': (me + k) % n_fsdp}, device_id_type=MESH)

    own_gain = pltpu.make_async_copy(gains_hbm, gains_all.at[me], gain_recv.at[0])
    own_gain.start()
    for k in range(1, n_fsdp):
        gain_copy(k, me).start()
    start_own(0)
    start_own(1)
    own_gain.wait()
    for k in range(1, n_fsdp):
        gain_copy(k, (me + n_fsdp - k) % n_fsdp).wait_recv()

    gains = gains_all[0]
    for k in range(1, n_fsdp):
        gains = gains + gains_all[k]
    g_rows = d_model // 128
    q_rows = q_rank // 128
    kv_rows = kv_rank // 128

    def norm_step(blk, carry):
        slot = blk % 2

        @pl.when(blk + 1 < n_blk)
        def _():
            x_copy(blk + 1, (blk + 1) % 2).start()

        x_copy(blk, slot).wait()
        row0 = pl.multiple_of(blk * BLOCK, BLOCK)
        for r in range(0, BLOCK, 32):
            xb = x_buf[slot, r:r + 32, :].astype(F32)
            inv = lax.rsqrt(jnp.sum(xb * xb, axis=-1, keepdims=True) * (1.0 / d_model) + EPSILON)
            for j in range(g_rows):
                a_buf[pl.ds(row0 + r, 32), j * 128:(j + 1) * 128] = (
                    xb[:, j * 128:(j + 1) * 128] * inv * gains[j:j + 1, :]).astype(BF16)
        return carry

    lax.fori_loop(0, n_blk, norm_step, 0)

    def tick_a(t):
        stage1(t)
        if t + 2 < n_units:
            start_own(t + 2)

    def tick_b(t):
        if 0 <= t - 1 < n_units:
            stage2(t - 1)
        if 0 <= t - 2 < n_units:
            stage3(t - 2)
        if 0 <= t - 3 < n_units:
            stage4(t - 3)

    for t in range(4):
        tick_a(t)
        tick_b(t)

    def lat_step(blk, carry):
        row0 = pl.multiple_of(blk * BLOCK, BLOCK)
        rows = pl.ds(row0, BLOCK)
        u = jnp.dot(a_buf[rows, :], w_dkv[...], preferred_element_type=F32)
        lat = u[:, :kv_rank]
        inv = lax.rsqrt(jnp.sum(lat * lat, axis=-1, keepdims=True) * (1.0 / kv_rank) + EPSILON)
        for j in range(kv_rows):
            lat_buf[rows, j * 128:(j + 1) * 128] = (
                lat[:, j * 128:(j + 1) * 128] * inv * gains[g_rows + q_rows + j:g_rows + q_rows + j + 1, :]).astype(BF16)
        pe = jnp.concatenate([u[:, kv_rank:], jnp.zeros((BLOCK, 128 - rope_dim), F32)], axis=-1)
        cs = jnp.concatenate([cos_r[...]] * (BLOCK // seq_len), axis=0)
        lo = jnp.concatenate([sin_lo[...]] * (BLOCK // seq_len), axis=0)
        hi = jnp.concatenate([sin_hi[...]] * (BLOCK // seq_len), axis=0)
        rot = pe * cs - pltpu.roll(pe, 128 - half, 1) * lo + pltpu.roll(pe, half, 1) * hi
        rot = rot.astype(BF16)
        pe_buf[rows, :] = rot[:, :rope_dim]
        rcomb[rows, :] = pltpu.roll(rot.astype(F32), nope, 1)
        return carry

    lax.fori_loop(0, n_blk, lat_step, 0)
    lat_out = pltpu.make_async_copy(lat_buf, lat_hbm, fin_sem.at[0])
    pe_out = pltpu.make_async_copy(pe_buf, pe_hbm, fin_sem.at[1])
    lat_out.start()
    pe_out.start()

    def qd_cut(j):
        def qd_step(blk, carry):
            rows = pl.ds(pl.multiple_of(blk * BLOCK, BLOCK), BLOCK)
            qd_buf[rows, j * cut:(j + 1) * cut] = jnp.dot(a_buf[rows, :], w_dq[j], preferred_element_type=F32)
            return carry

        lax.fori_loop(0, n_blk, qd_step, 0)

    for j in range(DQ_CUTS):
        tick_a(4 + j)
        tick_b(4 + j)
        qd_cut(j)

    def cq_step(blk, carry):
        rows = pl.ds(pl.multiple_of(blk * BLOCK, BLOCK), BLOCK)
        qd = qd_buf[rows, :]
        inv = lax.rsqrt(jnp.sum(qd * qd, axis=-1, keepdims=True) * (1.0 / q_rank) + EPSILON)
        for j in range(q_rows):
            cq_buf[rows, j * 128:(j + 1) * 128] = (
                qd[:, j * 128:(j + 1) * 128] * inv * gains[g_rows + j:g_rows + j + 1, :]).astype(BF16)
        return carry

    lax.fori_loop(0, n_blk, cq_step, 0)
    t_first = 4 + DQ_CUTS
    tick_a(t_first)
    tick_b(t_first)

    n_steps = GROUPS * n_blk
    span = n_blk // 2 + 1
    schedule = {}
    last = n_units + 2
    for i, t in enumerate(range(t_first + 1, last + 1)):
        if 5 * i + 1 < n_steps:
            schedule.setdefault(5 * i, []).append(functools.partial(tick_a, t) if t < n_units else None)
            schedule.setdefault(5 * i + 2, []).append(functools.partial(tick_b, t))
            done_tick = t
    n_pairs = heads_per_group // 2
    scale = head_q ** -0.5
    c2 = scale * math.log2(math.e)
    mask_val = -1e30 / scale

    def o_copy(g, row0, slot):
        return pltpu.make_async_copy(
            o_blk.at[slot], o_hbm.at[pl.ds(row0, BLOCK), pl.ds(pl.multiple_of(g * heads_per_group * v_dim, 128),
                                                              heads_per_group * v_dim)], o_sem.at[slot])

    def attn_step(step, carry):
        g = step // n_blk
        blk = step % n_blk
        slot = step % 2
        row0 = pl.multiple_of(blk * BLOCK, BLOCK)
        rows = pl.ds(row0, BLOCK)
        for at, fns in schedule.items():
            if any(fn is not None for fn in fns):
                @pl.when(step == at)
                def _():
                    for fn in fns:
                        if fn is not None:
                            fn()

        @pl.when(blk == 0)
        def _():
            for j in range(uq_cols // 128):
                wqt[j * 128:(j + 1) * 128, :] = w_uq[g, :, j * 128:(j + 1) * 128].T

        @pl.when(step >= 2)
        def _():
            o_copy(0, 0, slot).wait()

        qf[...] = nt_dot(wqt[...], cq_buf[rows, :])
        kvf = jnp.dot(lat_buf[rows, :], w_ukv[g], preferred_element_type=F32)
        lane = lax.broadcasted_iota(jnp.int32, (BLOCK, 128), 1)
        keep = lax.broadcasted_iota(jnp.int32, (seq_len, seq_len), 0) <= lax.broadcasted_iota(
            jnp.int32, (seq_len, seq_len), 1)
        ct, st = cos_t[...], sin_t[...]
        rc = rcomb[rows, :]
        for pair in range(n_pairs):
            outs = [[], []]
            for h in (2 * pair, 2 * pair + 1):
                q0 = h * head_q
                v1 = qf[q0 + nope:q0 + nope + half, :]
                v2 = qf[q0 + nope + half:q0 + head_q, :]
                q_aug = jnp.concatenate([
                    qf[q0:q0 + nope, :].astype(BF16),
                    (v1 * ct - v2 * st).astype(BF16),
                    (v2 * ct + v1 * st).astype(BF16),
                    jnp.zeros((128 - head_q, BLOCK), BF16)], axis=0)
                kvh = kvf[:, h * 128:(h + 1) * 128]
                k_aug = jnp.where(lane < nope, kvh, rc).astype(BF16)
                v_t = kvh.astype(BF16).T[nope:, :]
                for p in range(BLOCK // seq_len):
                    tok = slice(p * seq_len, (p + 1) * seq_len)
                    s_t = jnp.dot(k_aug[tok, :], q_aug[:, tok], preferred_element_type=F32)
                    s_t = jnp.where(keep, s_t, mask_val)
                    top = jnp.max(s_t, axis=0, keepdims=True)
                    e_t = jnp.exp2((s_t - top) * c2)
                    tot = jnp.sum(e_t, axis=0, keepdims=True)
                    p_t = (e_t * (1.0 / tot)).astype(BF16)
                    outs[p].append(jnp.dot(v_t[:, tok], p_t, preferred_element_type=F32))
            for p in range(BLOCK // seq_len):
                both = jnp.concatenate(outs[p], axis=0).astype(BF16)
                o_blk[slot, p * seq_len:(p + 1) * seq_len, pair * 128:(pair + 1) * 128] = both.T
        o_copy(g, row0, slot).start()
        return carry

    lax.fori_loop(0, n_steps, attn_step, 0)

    for t in range(done_tick + 1, last + 1):
        if t < n_units:
            tick_a(t)
        tick_b(t)
    outs = []
    for j in range(OUT_CUTS):
        cp = pltpu.make_async_copy(w_out.at[j], wout_hbm.at[:, pl.ds(j * out_cols, out_cols)], fin_sem.at[2 + j])
        cp.start()
        outs.append(cp)
    for slot in range(2):
        o_copy(0, 0, slot).wait()
    lat_out.wait()
    pe_out.wait()
    for unit in range(n_units):
        all_sent(unit)
    for k in range(1, n_fsdp):
        gain_copy(k, me).wait_send()
    for cp in outs:
        cp.wait()


def attention_part(x, gains, dq_s, uq_s, dkv_s, ukv_s, out_s, n_fsdp, seq_len, q_rank, kv_rank):
    n_tok, d_model = x.shape
    rope_dim = dkv_s.shape[1] - kv_rank
    v_total = out_s.shape[0] * n_fsdp
    nope_total = ukv_s.shape[1] - v_total
    n_heads = (uq_s.shape[1] - nope_total) // rope_dim
    nope, v_dim = nope_total // n_heads, v_total // n_heads
    hpg = n_heads // GROUPS
    half = rope_dim // 2
    cos_s, sin_s = rope_tables(seq_len, rope_dim)
    pad = jnp.zeros((seq_len, 128 - rope_dim), F32)
    zero = jnp.zeros((seq_len, half), F32)
    cos_r = jnp.concatenate([cos_s, cos_s, pad], axis=1)
    sin_lo = jnp.concatenate([sin_s, zero, pad], axis=1)
    sin_hi = jnp.concatenate([zero, sin_s, pad], axis=1)
    reps = BLOCK // seq_len
    cos_t = jnp.concatenate([cos_s.T] * reps, axis=1)
    sin_t = jnp.concatenate([sin_s.T] * reps, axis=1)
    dims = (n_fsdp, seq_len, kv_rank, rope_dim, nope, v_dim, hpg)
    n_pieces = 1 + DQ_CUTS + 2 * GROUPS + OUT_CUTS
    any_spec = pl.BlockSpec(memory_space=pl.ANY)
    vmem_spec = pl.BlockSpec(memory_space=pltpu.VMEM)
    dma = pltpu.SemaphoreType.DMA
    return pl.pallas_call(
        functools.partial(gather_kernel, dims),
        out_shape=(
            jax.ShapeDtypeStruct((n_tok, v_total), BF16),
            jax.ShapeDtypeStruct((n_tok, kv_rank), BF16),
            jax.ShapeDtypeStruct((n_tok, rope_dim), BF16),
            jax.ShapeDtypeStruct((v_total, d_model), BF16),
        ),
        in_specs=[any_spec] * 7 + [vmem_spec] * 5,
        out_specs=(any_spec,) * 4,
        scratch_shapes=[
            pltpu.VMEM((n_fsdp,) + gains.shape, F32),
            pltpu.VMEM((dkv_s.shape[0] * n_fsdp, dkv_s.shape[1]), BF16),
            pltpu.VMEM((DQ_CUTS, d_model, q_rank // DQ_CUTS), BF16),
            pltpu.VMEM((GROUPS, q_rank, uq_s.shape[1] // GROUPS), BF16),
            pltpu.VMEM((GROUPS, kv_rank, ukv_s.shape[1] // GROUPS), BF16),
            pltpu.VMEM((OUT_CUTS, v_total, d_model // OUT_CUTS), BF16),
            pltpu.VMEM((n_tok, d_model), BF16),
            pltpu.VMEM((n_tok, q_rank), F32),
            pltpu.VMEM((n_tok, q_rank), BF16),
            pltpu.VMEM((n_tok, kv_rank), BF16),
            pltpu.VMEM((n_tok, rope_dim), BF16),
            pltpu.VMEM((n_tok, 128), F32),
            pltpu.VMEM((2, BLOCK, d_model), BF16),
            pltpu.VMEM((hpg * (nope + rope_dim), q_rank), BF16),
            pltpu.VMEM((hpg * (nope + rope_dim), BLOCK), F32),
            pltpu.VMEM((2, BLOCK, hpg * v_dim), BF16),
            dma((n_pieces, N_KINDS)),
            dma((n_pieces, N_KINDS)),
            dma((n_pieces,)),
            dma((n_fsdp,)),
            dma((n_fsdp,)),
            dma((2,)),
            dma((2,)),
            dma((2 + OUT_CUTS,)),
        ],
        compiler_params=pltpu.CompilerParams(
            collective_id=0, has_side_effects=True, vmem_limit_bytes=67043328),
        name='latent_attention',
    )(x, gains, dq_s, uq_s, dkv_s, ukv_s, out_s, cos_r, sin_lo, sin_hi, cos_t, sin_t)


def solution(mesh):
    batch_spec = P(('dp', 'fsdp'))
    row_spec = P('fsdp')
    mat_spec = P('fsdp', None)
    n_fsdp = mesh.shape['fsdp']

    def run_block(tokens, gain_in, w_dq, gain_q, w_uq, w_dkv, gain_kv, w_ukv, w_out):
        seq_len = tokens.shape[1]

        def local_block(tok_blk, g_in, dq_s, g_q, uq_s, dkv_s, g_kv, ukv_s, out_s):
            n_prompts, _, d_model = tok_blk.shape
            me = lax.axis_index('fsdp')
            total = (g_in.shape[0] + g_q.shape[0] + g_kv.shape[0]) * n_fsdp
            rows = -(-total // 1024) * 8
            flat = jnp.zeros((rows * 128,), F32)
            start = 0
            for gain in (g_in, g_q, g_kv):
                flat = lax.dynamic_update_slice(flat, gain.astype(F32), (start + me * gain.shape[0],))
                start += gain.shape[0] * n_fsdp
            gains = flat.reshape(rows, 128)
            x = tok_blk.reshape(n_prompts * seq_len, d_model)
            attn_out, latent, k_pe, w_out_all = attention_part(
                x, gains, dq_s, uq_s, dkv_s, ukv_s, out_s, n_fsdp, seq_len, g_q.shape[0] * n_fsdp,
                g_kv.shape[0] * n_fsdp)
            proj = jnp.dot(attn_out, w_out_all, preferred_element_type=F32)
            y = (x.astype(F32) + proj).astype(BF16)
            return (y.reshape(tok_blk.shape), latent.reshape(n_prompts, seq_len, -1),
                    k_pe.reshape(n_prompts, seq_len, -1))

        mapped = jax.shard_map(
            local_block,
            mesh=mesh,
            in_specs=(batch_spec, row_spec, mat_spec, row_spec, mat_spec, mat_spec, row_spec, mat_spec, mat_spec),
            out_specs=(batch_spec, batch_spec, batch_spec),
            check_vma=False,
        )
        return mapped(tokens, gain_in, w_dq, gain_q, w_uq, w_dkv, gain_kv, w_ukv, w_out)

    return run_block
```

```python
import functools
import math

import jax
import jax.numpy as jnp
from jax import lax
from jax.experimental import pallas as pl
from jax.experimental.pallas import tpu as pltpu
from jax.sharding import PartitionSpec as P

EPSILON = 1e-6
ROPE_THETA = 10000.0
BF16 = jnp.bfloat16
F32 = jnp.float32
MESH = pl.DeviceIdType.MESH

SPLIT = {320: (112, 96), 96: (32, 32), 32: (16, 0)}
N_KINDS = 11
GROUPS = 5
DQ_CUTS = 3
OUT_CUTS = 5
BLOCK = 256


def rope_tables(seq_len, rope_dim):
    half_dim = rope_dim // 2
    inv_freq = ROPE_THETA ** (-2.0 * jnp.arange(half_dim, dtype=F32) / rope_dim)
    angles = jnp.arange(seq_len, dtype=F32)[:, None] * inv_freq[None, :]
    return jnp.cos(angles), jnp.sin(angles)


def nt_dot(lhs, rhs):
    return lax.dot_general(lhs, rhs, (((1,), (1,)), ((), ())), preferred_element_type=F32)


class Piece:
    def __init__(self, base, src, dst, rows):
        self.base, self.src, self.dst, self.rows = base, src, dst, rows
        self.m, self.c = SPLIT[rows]


def gather_kernel(dims, x_hbm, gains_hbm, dq_hbm, uq_hbm, dkv_hbm, ukv_hbm, out_hbm,
                  cos_r, sin_lo, sin_hi, cos_t, sin_t,
                  o_hbm, lat_hbm, pe_hbm, wout_hbm,
                  gains_all, w_dkv, w_dq, w_uq, w_ukv, w_out,
                  a_buf, qd_buf, cq_buf, lat_buf, pe_buf, rcomb, u_buf, wqt, wk, wvt, qf, kf, vt, sbuf, o_blk,
                  send_sem, recv_sem, own_sem, gain_send, gain_recv, x_sem, o_sem, fin_sem):
    n_fsdp, seq_len, kv_rank, rope_dim, nope, v_dim, heads_per_group = dims
    half = rope_dim // 2
    head_q = nope + rope_dim
    n_tok, d_model = a_buf.shape
    n_blk = n_tok // BLOCK
    q_rank = cq_buf.shape[1]
    me = lax.axis_index('fsdp')
    dp = lax.axis_index('dp')
    n_x = n_fsdp // 2
    core = me % 2
    xx = me // 2
    right = ((xx + 1) % n_x) * 2 + core
    left = ((xx + n_x - 1) % n_x) * 2 + core
    far = ((xx + 2) % n_x) * 2 + core
    mate = xx * 2 + 1 - core
    par = dp % 2
    dp_mate = dp + 1 - 2 * par

    barrier = pltpu.get_barrier_semaphore()
    for k in range(1, n_fsdp):
        pl.semaphore_signal(barrier, inc=1, device_id={'fsdp': (me + k) % n_fsdp}, device_id_type=MESH)
    pl.semaphore_signal(barrier, inc=1, device_id={'dp': dp_mate}, device_id_type=MESH)

    def x_copy(blk):
        rows = pl.ds(pl.multiple_of(blk * BLOCK, BLOCK), BLOCK)
        return pltpu.make_async_copy(x_hbm.at[rows, :], a_buf.at[rows, :], x_sem.at[blk])

    for blk in range(n_blk):
        x_copy(blk).start()

    def rows_of(ref, owner, rows, off, count, cols=None):
        start = pl.multiple_of(owner * rows + off, 16)
        return ref.at[pl.ds(start, count), :]

    pieces = {}
    base = [0]

    def add(unit, src, dst, rows):
        pieces.setdefault(unit, []).append(Piece(base[0], src, dst, rows))
        base[0] += 1

    add(0, dkv_hbm, w_dkv, dkv_hbm.shape[0])
    cut = q_rank // DQ_CUTS
    for j in range(DQ_CUTS):
        add(1 + j, dq_hbm.at[:, pl.ds(j * cut, cut)], w_dq.at[j], dq_hbm.shape[0])
    uq_cols, ukv_cols = heads_per_group * head_q, heads_per_group * (nope + v_dim)
    for g in range(GROUPS):
        add(1 + DQ_CUTS + g, uq_hbm.at[:, pl.ds(g * uq_cols, uq_cols)], w_uq.at[g], uq_hbm.shape[0])
        add(1 + DQ_CUTS + g, ukv_hbm.at[:, pl.ds(g * ukv_cols, ukv_cols)], w_ukv.at[g], ukv_hbm.shape[0])
    out_cols = out_hbm.shape[1] // OUT_CUTS
    for j in range(OUT_CUTS):
        add(1 + DQ_CUTS + GROUPS + j, out_hbm.at[:, pl.ds(j * out_cols, out_cols)], w_out.at[j], out_hbm.shape[0])
    n_units = 1 + DQ_CUTS + GROUPS + OUT_CUTS

    def copy(p, kind, owner, off, count, to, from_own=False):
        start = pl.multiple_of(off, 16) if not isinstance(off, int) else off
        dst = rows_of(p.dst, owner, p.rows, off, count)
        src = p.src.at[pl.ds(start, count), :] if from_own else dst
        return pltpu.make_async_remote_copy(
            src_ref=src, dst_ref=dst, send_sem=send_sem.at[p.base, kind], recv_sem=recv_sem.at[p.base, kind],
            device_id=to, device_id_type=MESH)

    def geom(p):
        edge = p.rows - p.m - p.c
        x_off = par * edge
        m_off = par * (p.rows - p.m)
        z_off = (1 - par) * (p.rows - p.m)
        return x_off, m_off, z_off

    to_right, to_left, to_mate, to_dp = {'fsdp': right}, {'fsdp': left}, {'fsdp': mate}, {'dp': dp_mate}
    mate_of = lambda owner: owner + 1 - 2 * core

    def own_copy(p):
        return pltpu.make_async_copy(p.src, rows_of(p.dst, me, p.rows, 0, p.rows), own_sem.at[p.base])

    def start_own(unit):
        for p in pieces[unit]:
            x_off, _, _ = geom(p)
            copy(p, 0, me, x_off, p.m + p.c, to_right, True).start()
            copy(p, 1, me, x_off, p.m + p.c, to_left, True).start()
            copy(p, 7, me, 0, p.rows, to_mate, True).start()
            own_copy(p).start()

    def stage1(unit):
        for p in pieces[unit]:
            x_off, m_off, _ = geom(p)
            copy(p, 0, left, x_off, p.m + p.c, to_right).wait_recv()
            copy(p, 2, left, m_off, p.m, to_right).start()
            copy(p, 4, left, m_off, p.m, to_dp).start()
            copy(p, 1, right, x_off, p.m + p.c, to_left).wait_recv()
            if p.c:
                copy(p, 3, right, p.m, p.c, to_left).start()
            copy(p, 5, right, m_off, p.m, to_dp).start()

    def stage2(unit):
        for p in pieces[unit]:
            _, m_off, _ = geom(p)
            copy(p, 2, far, m_off, p.m, to_right).wait_recv()
            copy(p, 6, far, m_off, p.m, to_dp).start()
            if p.c:
                copy(p, 3, far, p.m, p.c, to_left).wait_recv()

    def stage3(unit):
        for p in pieces[unit]:
            _, _, z_off = geom(p)
            for kind, owner in ((4, left), (5, right), (6, far)):
                copy(p, kind, owner, z_off, p.m, to_dp).wait_recv()
                copy(p, kind + 4, owner, 0, p.rows, to_mate).start()

    def stage4(unit):
        for p in pieces[unit]:
            for kind, owner in ((7, me), (8, left), (9, right), (10, far)):
                copy(p, kind, mate_of(owner), 0, p.rows, to_mate).wait_recv()
            own_copy(p).wait()

    def all_sent(unit):
        for p in pieces[unit]:
            x_off, m_off, _ = geom(p)
            copy(p, 0, me, x_off, p.m + p.c, to_right, True).wait_send()
            copy(p, 1, me, x_off, p.m + p.c, to_left, True).wait_send()
            copy(p, 2, left, m_off, p.m, to_right).wait_send()
            if p.c:
                copy(p, 3, right, p.m, p.c, to_left).wait_send()
            for kind, owner in ((4, left), (5, right), (6, far)):
                copy(p, kind, owner, m_off, p.m, to_dp).wait_send()
            copy(p, 7, me, 0, p.rows, to_mate, True).wait_send()
            for kind, owner in ((8, left), (9, right), (10, far)):
                copy(p, kind, owner, 0, p.rows, to_mate).wait_send()

    pl.semaphore_wait(barrier, n_fsdp)

    def gain_copy(k, owner):
        return pltpu.make_async_remote_copy(
            src_ref=gains_hbm, dst_ref=gains_all.at[owner], send_sem=gain_send.at[k], recv_sem=gain_recv.at[k],
            device_id={'fsdp': (me + k) % n_fsdp}, device_id_type=MESH)

    own_gain = pltpu.make_async_copy(gains_hbm, gains_all.at[me], gain_recv.at[0])
    own_gain.start()
    for k in range(1, n_fsdp):
        gain_copy(k, me).start()
    start_own(0)
    start_own(1)
    own_gain.wait()
    for k in range(1, n_fsdp):
        gain_copy(k, (me + n_fsdp - k) % n_fsdp).wait_recv()

    lane_row = lax.broadcasted_iota(jnp.int32, (1, 128), 1)
    gain_rows = [None] * ((d_model + q_rank + kv_rank) // 128)

    def put(row, value):
        gain_rows[row] = value if gain_rows[row] is None else gain_rows[row] + value

    for owner in range(n_fsdp):
        base_row, local_row = 0, 0
        for total in (d_model, q_rank, kv_rank):
            count = total // n_fsdp
            for r in range(-(-count // 128)):
                size = min(128, count - 128 * r)
                at = owner * count + 128 * r
                row, off = base_row + at // 128, at % 128
                value = gains_all[owner, local_row:local_row + 1, :]
                if off:
                    value = pltpu.roll(value, off, 1)
                    put(row, jnp.where(lane_row >= off, value, 0.0))
                    if off + size > 128:
                        put(row + 1, jnp.where(lane_row < off, value, 0.0))
                else:
                    put(row, value)
                local_row += 1
            base_row += total // 128
    gains = jnp.concatenate(gain_rows, axis=0)
    g_rows = d_model // 128
    q_rows = q_rank // 128
    kv_rows = kv_rank // 128

    def norm_step(blk, carry):
        x_copy(blk).wait()
        row0 = pl.multiple_of(blk * BLOCK, BLOCK)
        for r in range(0, BLOCK, 32):
            xb = a_buf[pl.ds(row0 + r, 32), :].astype(F32)
            inv = lax.rsqrt(jnp.sum(xb * xb, axis=-1, keepdims=True) * (1.0 / d_model) + EPSILON)
            for j in range(g_rows):
                a_buf[pl.ds(row0 + r, 32), j * 128:(j + 1) * 128] = (
                    xb[:, j * 128:(j + 1) * 128] * inv * gains[j:j + 1, :]).astype(BF16)
        return carry

    def tick_a(t):
        stage1(t)
        if t + 2 < n_units:
            start_own(t + 2)

    def lat_step(blk, carry):
        rows = pl.ds(pl.multiple_of(blk * 2 * BLOCK, BLOCK), 2 * BLOCK)
        u_buf[rows, :] = jnp.dot(a_buf[rows, :], w_dkv[...], preferred_element_type=F32)
        return carry

    def lat_finish(blk):
        rows = pl.ds(pl.multiple_of(blk * BLOCK, BLOCK), BLOCK)
        lat = u_buf[rows, :kv_rank]
        inv = lax.rsqrt(jnp.sum(lat * lat, axis=-1, keepdims=True) * (1.0 / kv_rank) + EPSILON)
        for j in range(kv_rows):
            lat_buf[rows, j * 128:(j + 1) * 128] = (
                lat[:, j * 128:(j + 1) * 128] * inv * gains[g_rows + q_rows + j:g_rows + q_rows + j + 1, :]).astype(BF16)
        pe = jnp.concatenate([u_buf[rows, kv_rank:], jnp.zeros((BLOCK, 128 - rope_dim), F32)], axis=-1)
        cs = jnp.concatenate([cos_r[...]] * (BLOCK // seq_len), axis=0)
        lo = jnp.concatenate([sin_lo[...]] * (BLOCK // seq_len), axis=0)
        hi = jnp.concatenate([sin_hi[...]] * (BLOCK // seq_len), axis=0)
        rot = pe * cs - pltpu.roll(pe, 128 - half, 1) * lo + pltpu.roll(pe, half, 1) * hi
        rot = rot.astype(BF16)
        pe_buf[rows, :] = rot[:, :rope_dim]
        rcomb[rows, :] = rot

    def run(fn, lo, hi):
        lax.fori_loop(lo, hi, fn, 0)

    run(norm_step, 0, 6)
    tick_a(0)
    run(norm_step, 6, n_blk)
    tick_a(1)
    stage2(0)
    tick_a(2)
    stage2(1)
    stage3(0)
    tick_a(3)
    stage4(0)
    stage2(2)
    half_blk = n_blk // 2
    run(lat_step, 0, 1)
    stage3(1)
    run(lat_step, 1, 2)
    tick_a(4)
    stage2(3)
    run(lat_step, 2, 3)
    stage3(2)
    run(lat_step, 3, half_blk)
    tick_a(5)
    def qd_cut(j, lo, hi):
        def qd_step(blk, carry):
            rows = pl.ds(pl.multiple_of(blk * 2 * BLOCK, BLOCK), 2 * BLOCK)
            qd_buf[rows, j * cut:(j + 1) * cut] = jnp.dot(a_buf[rows, :], w_dq[j], preferred_element_type=F32)
            if j == 0:
                lat_finish(2 * blk)
                lat_finish(2 * blk + 1)
            return carry

        lax.fori_loop(lo, hi, qd_step, 0)

    mid = half_blk // 2
    stage2(4)
    stage4(1)
    qd_cut(0, 0, mid)
    stage3(3)
    qd_cut(0, mid, half_blk)
    lat_out = pltpu.make_async_copy(lat_buf, lat_hbm, fin_sem.at[0])
    pe_out = pltpu.make_async_copy(pe_buf, pe_hbm, fin_sem.at[1])
    lat_out.start()
    pe_out.start()

    tick_a(6)
    stage4(2)
    qd_cut(1, 0, mid)
    stage2(5)
    qd_cut(1, mid, half_blk)
    stage3(4)
    stage4(3)
    qd_cut(2, 0, mid)
    tick_a(7)
    qd_cut(2, mid, half_blk)
    stage2(6)
    stage3(5)

    def cq_step(blk, carry):
        rows = pl.ds(pl.multiple_of(blk * BLOCK, BLOCK), BLOCK)
        qd = qd_buf[rows, :]
        inv = lax.rsqrt(jnp.sum(qd * qd, axis=-1, keepdims=True) * (1.0 / q_rank) + EPSILON)
        for j in range(q_rows):
            cq_buf[rows, j * 128:(j + 1) * 128] = (
                qd[:, j * 128:(j + 1) * 128] * inv * gains[g_rows + j:g_rows + j + 1, :]).astype(BF16)
        return carry

    lax.fori_loop(0, n_blk, cq_step, 0)
    stage4(4)

    n_steps = GROUPS * n_blk

    def out_copy(j):
        return pltpu.make_async_copy(w_out.at[j], wout_hbm.at[:, pl.ds(j * out_cols, out_cols)], fin_sem.at[2 + j])

    first_out = 1 + DQ_CUTS + GROUPS

    def finish_out(unit):
        stage4(unit)
        out_copy(unit - first_out).start()

    plan = [(0, tick_a, 8), (1, stage2, 7), (1, stage3, 6), (3, stage2, 8), (4, stage3, 7), (5, tick_a, 9),
            (7, stage3, 8), (8, stage4, 5), (8, stage2, 9), (10, tick_a, 10), (12, stage3, 9), (13, stage2, 10),
            (15, tick_a, 11), (15, finish_out, 9), (16, stage4, 6), (17, stage3, 10), (18, stage2, 11),
            (20, tick_a, 12), (20, finish_out, 10), (22, stage3, 11), (23, stage2, 12), (24, stage4, 7),
            (25, tick_a, 13), (25, finish_out, 11), (27, stage3, 12), (28, stage2, 13), (30, finish_out, 12),
            (32, stage4, 8), (33, stage3, 13), (36, finish_out, 13)]
    schedule = {}
    for at, fn, unit in plan:
        schedule.setdefault(at, []).append((fn, unit))
    n_pairs = heads_per_group // 2
    scale = head_q ** -0.5
    c2 = scale * math.log2(math.e)
    mask_val = -1e30 / scale

    def o_copy(g, row0, slot):
        return pltpu.make_async_copy(
            o_blk.at[slot], o_hbm.at[pl.ds(row0, BLOCK), pl.ds(pl.multiple_of(g * heads_per_group * v_dim, 128),
                                                              heads_per_group * v_dim)], o_sem.at[slot])

    def attn_step(step, carry):
        g = step // n_blk
        blk = step % n_blk
        slot = step % 2
        row0 = pl.multiple_of(blk * BLOCK, BLOCK)
        rows = pl.ds(row0, BLOCK)
        for part in range(GROUPS):
            @pl.when(g == part)
            def _():
                for at, todo in schedule.items():
                    if at // n_blk == part:
                        @pl.when(step == at)
                        def _():
                            for fn, unit in todo:
                                fn(unit)

        @pl.when(blk == 0)
        def _():
            for j in range(uq_cols // 128):
                wqt[j * 128:(j + 1) * 128, :] = w_uq[g, :, j * 128:(j + 1) * 128].T
            low = lax.broadcasted_iota(jnp.int32, (kv_rank, 128), 1) < nope
            for j in range(n_pairs):
                even = w_ukv[g, :, (2 * j) * 128:(2 * j + 1) * 128].astype(F32)
                odd = w_ukv[g, :, (2 * j + 1) * 128:(2 * j + 2) * 128].astype(F32)
                wk[:, j * 128:(j + 1) * 128] = jnp.where(low, even, pltpu.roll(odd, nope, 1)).astype(BF16)
                wvt[j * 128:(j + 1) * 128, :] = jnp.where(low, pltpu.roll(even, nope, 1), odd).astype(BF16).T

        @pl.when(step >= 2)
        def _():
            o_copy(0, 0, slot).wait()

        @pl.when(step < n_steps)
        def _():
            qf[...] = nt_dot(wqt[...], cq_buf[rows, :])
            kf[...] = jnp.dot(lat_buf[rows, :], wk[...], preferred_element_type=F32).astype(BF16)
            vt[...] = nt_dot(wvt[...], lat_buf[rows, :]).astype(BF16)

        keep = lax.broadcasted_iota(jnp.int32, (seq_len, 2 * seq_len), 0) <= lax.broadcasted_iota(
            jnp.int32, (seq_len, 2 * seq_len), 1) % seq_len
        ct, st = cos_t[...], sin_t[...]
        rc = rcomb[rows, :]
        zero = jnp.zeros((nope, seq_len), BF16)
        tail = jnp.zeros((128 - rope_dim, 2 * seq_len), BF16)
        @pl.when(step < n_steps)
        def _():
            for pair in range(n_pairs):
                q_nope, q_pe = [], []
                for h in (2 * pair, 2 * pair + 1):
                    q0 = h * head_q
                    v1 = qf[q0 + nope:q0 + nope + half, :]
                    v2 = qf[q0 + nope + half:q0 + head_q, :]
                    q_nope.append(qf[q0:q0 + nope, :].astype(BF16))
                    q_pe.append(jnp.concatenate([(v1 * ct - v2 * st).astype(BF16), (v2 * ct + v1 * st).astype(BF16)], axis=0))
                cols = slice(pair * 128, (pair + 1) * 128)
                for p in range(BLOCK // seq_len):
                    tok = slice(p * seq_len, (p + 1) * seq_len)
                    k_all = jnp.concatenate([kf[tok, cols], rc[tok, :]], axis=1)
                    q_all = jnp.concatenate([
                        jnp.concatenate([q_nope[0][:, tok], zero], axis=1),
                        jnp.concatenate([zero, q_nope[1][:, tok]], axis=1),
                        jnp.concatenate([q_pe[0][:, tok], q_pe[1][:, tok]], axis=1),
                        tail], axis=0)
                    sbuf[2 * pair + p] = jnp.dot(k_all, q_all, preferred_element_type=F32)

        @pl.when(step < n_steps)
        def _():
            for pair in range(n_pairs):
                cols = slice(pair * 128, (pair + 1) * 128)
                for p in range(BLOCK // seq_len):
                    tok = slice(p * seq_len, (p + 1) * seq_len)
                    s_t = sbuf[2 * pair + p]
                    s_t = jnp.where(keep, s_t, mask_val)
                    top = jnp.max(s_t, axis=0, keepdims=True)
                    e_t = jnp.exp2((s_t - top) * c2)
                    tot = jnp.sum(e_t, axis=0, keepdims=True)
                    p_t = (e_t * (1.0 / tot)).astype(BF16)
                    both = jnp.dot(vt[cols, tok], p_t, preferred_element_type=F32)
                    both = jnp.concatenate([both[:v_dim, :seq_len], both[v_dim:, seq_len:]], axis=0)
                    o_blk[slot, tok, cols] = both.astype(BF16).T
        o_copy(g, row0, slot).start()
        return carry

    lax.fori_loop(0, n_steps, attn_step, 0)

    for slot in range(2):
        o_copy(0, 0, slot).wait()
    lat_out.wait()
    pe_out.wait()
    for unit in range(n_units):
        all_sent(unit)
    for k in range(1, n_fsdp):
        gain_copy(k, me).wait_send()
    for j in range(OUT_CUTS):
        out_copy(j).wait()


def attention_part(x, gains, dq_s, uq_s, dkv_s, ukv_s, out_s, n_fsdp, seq_len, q_rank, kv_rank):
    n_tok, d_model = x.shape
    rope_dim = dkv_s.shape[1] - kv_rank
    v_total = out_s.shape[0] * n_fsdp
    nope_total = ukv_s.shape[1] - v_total
    n_heads = (uq_s.shape[1] - nope_total) // rope_dim
    nope, v_dim = nope_total // n_heads, v_total // n_heads
    hpg = n_heads // GROUPS
    half = rope_dim // 2
    cos_s, sin_s = rope_tables(seq_len, rope_dim)
    pad = jnp.zeros((seq_len, 128 - rope_dim), F32)
    zero = jnp.zeros((seq_len, half), F32)
    cos_r = jnp.concatenate([cos_s, cos_s, pad], axis=1)
    sin_lo = jnp.concatenate([sin_s, zero, pad], axis=1)
    sin_hi = jnp.concatenate([zero, sin_s, pad], axis=1)
    reps = BLOCK // seq_len
    cos_t = jnp.concatenate([cos_s.T] * reps, axis=1)
    sin_t = jnp.concatenate([sin_s.T] * reps, axis=1)
    dims = (n_fsdp, seq_len, kv_rank, rope_dim, nope, v_dim, hpg)
    n_pieces = 1 + DQ_CUTS + 2 * GROUPS + OUT_CUTS
    any_spec = pl.BlockSpec(memory_space=pl.ANY)
    vmem_spec = pl.BlockSpec(memory_space=pltpu.VMEM)
    dma = pltpu.SemaphoreType.DMA
    return pl.pallas_call(
        functools.partial(gather_kernel, dims),
        out_shape=(
            jax.ShapeDtypeStruct((n_tok, v_total), BF16),
            jax.ShapeDtypeStruct((n_tok, kv_rank), BF16),
            jax.ShapeDtypeStruct((n_tok, rope_dim), BF16),
            jax.ShapeDtypeStruct((v_total, d_model), BF16),
        ),
        in_specs=[any_spec] * 7 + [vmem_spec] * 5,
        out_specs=(any_spec,) * 4,
        scratch_shapes=[
            pltpu.VMEM((n_fsdp,) + gains.shape, F32),
            pltpu.VMEM((dkv_s.shape[0] * n_fsdp, dkv_s.shape[1]), BF16),
            pltpu.VMEM((DQ_CUTS, d_model, q_rank // DQ_CUTS), BF16),
            pltpu.VMEM((GROUPS, q_rank, uq_s.shape[1] // GROUPS), BF16),
            pltpu.VMEM((GROUPS, kv_rank, ukv_s.shape[1] // GROUPS), BF16),
            pltpu.VMEM((OUT_CUTS, v_total, d_model // OUT_CUTS), BF16),
            pltpu.VMEM((n_tok, d_model), BF16),
            pltpu.VMEM((n_tok, q_rank), F32),
            pltpu.VMEM((n_tok, q_rank), BF16),
            pltpu.VMEM((n_tok, kv_rank), BF16),
            pltpu.VMEM((n_tok, rope_dim), BF16),
            pltpu.VMEM((n_tok, 128), BF16),
            pltpu.VMEM((n_tok, dkv_s.shape[1]), F32),
            pltpu.VMEM((hpg * (nope + rope_dim), q_rank), BF16),
            pltpu.VMEM((kv_rank, hpg * nope), BF16),
            pltpu.VMEM((hpg * v_dim, kv_rank), BF16),
            pltpu.VMEM((hpg * (nope + rope_dim), BLOCK), F32),
            pltpu.VMEM((BLOCK, hpg * nope), BF16),
            pltpu.VMEM((hpg * v_dim, BLOCK), BF16),
            pltpu.VMEM((hpg, 128, 256), F32),
            pltpu.VMEM((2, BLOCK, hpg * v_dim), BF16),
            dma((n_pieces, N_KINDS)),
            dma((n_pieces, N_KINDS)),
            dma((n_pieces,)),
            dma((n_fsdp,)),
            dma((n_fsdp,)),
            dma((n_tok // BLOCK,)),
            dma((2,)),
            dma((2 + OUT_CUTS,)),
        ],
        compiler_params=pltpu.CompilerParams(
            collective_id=0, has_side_effects=True, vmem_limit_bytes=67043328),
        name='latent_attention',
    )(x, gains, dq_s, uq_s, dkv_s, ukv_s, out_s, cos_r, sin_lo, sin_hi, cos_t, sin_t)


def solution(mesh):
    batch_spec = P(('dp', 'fsdp'))
    row_spec = P('fsdp')
    mat_spec = P('fsdp', None)
    n_fsdp = mesh.shape['fsdp']

    def run_block(tokens, gain_in, w_dq, gain_q, w_uq, w_dkv, gain_kv, w_ukv, w_out):
        seq_len = tokens.shape[1]

        def local_block(tok_blk, g_in, dq_s, g_q, uq_s, dkv_s, g_kv, ukv_s, out_s):
            n_prompts, _, d_model = tok_blk.shape
            parts = [jnp.pad(g.astype(F32), (0, -g.shape[0] % 128)) for g in (g_in, g_q, g_kv)]
            flat = jnp.concatenate(parts)
            gains = jnp.pad(flat, (0, -flat.shape[0] % 1024)).reshape(-1, 128)
            x = tok_blk.reshape(n_prompts * seq_len, d_model)
            attn_out, latent, k_pe, w_out_all = attention_part(
                x, gains, dq_s, uq_s, dkv_s, ukv_s, out_s, n_fsdp, seq_len, g_q.shape[0] * n_fsdp,
                g_kv.shape[0] * n_fsdp)
            proj = jnp.dot(attn_out, w_out_all, preferred_element_type=F32)
            y = (x.astype(F32) + proj).astype(BF16)
            return (y.reshape(tok_blk.shape), latent.reshape(n_prompts, seq_len, -1),
                    k_pe.reshape(n_prompts, seq_len, -1))

        mapped = jax.shard_map(
            local_block,
            mesh=mesh,
            in_specs=(batch_spec, row_spec, mat_spec, row_spec, mat_spec, mat_spec, row_spec, mat_spec, mat_spec),
            out_specs=(batch_spec, batch_spec, batch_spec),
            check_vma=False,
        )
        return mapped(tokens, gain_in, w_dq, gain_q, w_uq, w_dkv, gain_kv, w_ukv, w_out)

    return run_block
```

```python
import functools
import math

import jax
import jax.numpy as jnp
import numpy as np
from jax import lax
from jax.experimental import pallas as pl
from jax.experimental.pallas import tpu as pltpu
from jax.sharding import PartitionSpec as P

EPSILON = 1e-6
ROPE_THETA = 10000.0
BF16 = jnp.bfloat16
F32 = jnp.float32
MESH = pl.DeviceIdType.MESH

SPLIT = {320: (112, 96), 96: (32, 32), 32: (16, 0)}
OUT_SPLIT = (96, 128)
N_KINDS = 11
GROUPS = 5
DQ_CUTS = 3
OUT_CUTS = 5
BLOCK = 256
TALL = 512
AHEAD = {12: (), 13: ()}


def rope_tables(seq_len, rope_dim):
    half_dim = rope_dim // 2
    inv_freq = ROPE_THETA ** (-2.0 * np.arange(half_dim) / rope_dim)
    angles = np.arange(seq_len)[:, None] * inv_freq[None, :]
    return np.cos(angles).astype(np.float32), np.sin(angles).astype(np.float32)


def nt_dot(lhs, rhs):
    return lax.dot_general(lhs, rhs, (((1,), (1,)), ((), ())), preferred_element_type=F32)


class Piece:
    def __init__(self, base, src, dst, rows, split):
        self.base, self.src, self.dst, self.rows = base, src, dst, rows
        self.m, self.c = split or SPLIT[rows]


def gather_kernel(dims, x_hbm, gains_hbm, dq_hbm, uq_hbm, dkv_hbm, ukv_hbm, out_hbm,
                  tab_r_hbm, tab_t_hbm,
                  o_hbm, lat_hbm, pe_hbm, wout_hbm,
                  tab_r, tab_t, gains_all, w_dkv, w_dq, w_uq, w_ukv, w_out,
                  a_buf, qd_buf, cq_buf, lat_buf, pe_buf, rcomb, u_buf, wqt, wk, wvt, qf, kf, vt, sbuf, o_blk,
                  send_sem, recv_sem, own_sem, gain_send, gain_recv, x_sem, o_sem, fin_sem, tab_sem):
    n_fsdp, seq_len, kv_rank, rope_dim, nope, v_dim, heads_per_group = dims
    half = rope_dim // 2
    head_q = nope + rope_dim
    n_tok, d_model = a_buf.shape
    n_blk = n_tok // BLOCK
    q_rank = cq_buf.shape[1]
    me = lax.axis_index('fsdp')
    dp = lax.axis_index('dp')
    n_x = n_fsdp // 2
    core = me % 2
    xx = me // 2
    right = ((xx + 1) % n_x) * 2 + core
    left = ((xx + n_x - 1) % n_x) * 2 + core
    far = ((xx + 2) % n_x) * 2 + core
    mate = xx * 2 + 1 - core
    par = dp % 2
    dp_mate = dp + 1 - 2 * par

    barrier = pltpu.get_barrier_semaphore()
    for k in range(1, n_fsdp):
        pl.semaphore_signal(barrier, inc=1, device_id={'fsdp': (me + k) % n_fsdp}, device_id_type=MESH)
    pl.semaphore_signal(barrier, inc=1, device_id={'dp': dp_mate}, device_id_type=MESH)

    def x_copy(blk):
        rows = pl.ds(pl.multiple_of(blk * BLOCK, BLOCK), BLOCK)
        return pltpu.make_async_copy(x_hbm.at[rows, :], a_buf.at[rows, :], x_sem.at[blk])

    for blk in range(n_blk):
        x_copy(blk).start()
    tab_copies = (pltpu.make_async_copy(tab_r_hbm, tab_r, tab_sem.at[0]),
                  pltpu.make_async_copy(tab_t_hbm, tab_t, tab_sem.at[1]))
    for cp in tab_copies:
        cp.start()
    cos_r, sin_lo, sin_hi = tab_r.at[0], tab_r.at[1], tab_r.at[2]
    cos_t, sin_t = tab_t.at[0], tab_t.at[1]

    def rows_of(ref, owner, rows, off, count, cols=None):
        start = pl.multiple_of(owner * rows + off, 16)
        return ref.at[pl.ds(start, count), :]

    pieces = {}
    base = [0]

    def add(unit, src, dst, rows, split=None):
        pieces.setdefault(unit, []).append(Piece(base[0], src, dst, rows, split))
        base[0] += 1

    add(0, dkv_hbm, w_dkv, dkv_hbm.shape[0])
    cut = q_rank // DQ_CUTS
    for j in range(DQ_CUTS):
        add(1 + j, dq_hbm.at[:, pl.ds(j * cut, cut)], w_dq.at[j], dq_hbm.shape[0])
    uq_cols, ukv_cols = heads_per_group * head_q, heads_per_group * (nope + v_dim)
    for g in range(GROUPS):
        add(1 + DQ_CUTS + g, uq_hbm.at[:, pl.ds(g * uq_cols, uq_cols)], w_uq.at[g], uq_hbm.shape[0])
        add(1 + DQ_CUTS + g, ukv_hbm.at[:, pl.ds(g * ukv_cols, ukv_cols)], w_ukv.at[g], ukv_hbm.shape[0])
    out_cols = out_hbm.shape[1] // OUT_CUTS
    for j in range(OUT_CUTS):
        add(1 + DQ_CUTS + GROUPS + j, out_hbm.at[:, pl.ds(j * out_cols, out_cols)], w_out.at[j], out_hbm.shape[0], OUT_SPLIT)
    n_units = 1 + DQ_CUTS + GROUPS + OUT_CUTS

    def copy(p, kind, owner, off, count, to, from_own=False):
        start = pl.multiple_of(off, 16) if not isinstance(off, int) else off
        dst = rows_of(p.dst, owner, p.rows, off, count)
        src = p.src.at[pl.ds(start, count), :] if from_own else dst
        return pltpu.make_async_remote_copy(
            src_ref=src, dst_ref=dst, send_sem=send_sem.at[p.base, kind], recv_sem=recv_sem.at[p.base, kind],
            device_id=to, device_id_type=MESH)

    def geom(p):
        edge = p.rows - p.m - p.c
        x_off = par * edge
        m_off = par * (p.rows - p.m)
        z_off = (1 - par) * (p.rows - p.m)
        return x_off, m_off, z_off

    to_right, to_left, to_mate, to_dp = {'fsdp': right}, {'fsdp': left}, {'fsdp': mate}, {'dp': dp_mate}
    mate_of = lambda owner: owner + 1 - 2 * core

    def own_copy(p):
        return pltpu.make_async_copy(p.src, rows_of(p.dst, me, p.rows, 0, p.rows), own_sem.at[p.base])

    def start_own(unit):
        for p in pieces[unit]:
            x_off, _, _ = geom(p)
            copy(p, 0, me, x_off, p.m + p.c, to_right, True).start()
            copy(p, 1, me, x_off, p.m + p.c, to_left, True).start()
            copy(p, 7, me, 0, p.rows, to_mate, True).start()
            own_copy(p).start()

    def stage1(unit):
        for p in pieces[unit]:
            x_off, m_off, _ = geom(p)
            copy(p, 0, left, x_off, p.m + p.c, to_right).wait_recv()
            copy(p, 2, left, m_off, p.m, to_right).start()
            copy(p, 4, left, m_off, p.m, to_dp).start()
            copy(p, 1, right, x_off, p.m + p.c, to_left).wait_recv()
            if p.c:
                copy(p, 3, right, p.m, p.c, to_left).start()
            copy(p, 5, right, m_off, p.m, to_dp).start()

    def stage2(unit):
        for p in pieces[unit]:
            _, m_off, _ = geom(p)
            copy(p, 2, far, m_off, p.m, to_right).wait_recv()
            copy(p, 6, far, m_off, p.m, to_dp).start()
            if p.c:
                copy(p, 3, far, p.m, p.c, to_left).wait_recv()

    def stage3(unit):
        for p in pieces[unit]:
            _, _, z_off = geom(p)
            for kind, owner in ((4, left), (5, right), (6, far)):
                copy(p, kind, owner, z_off, p.m, to_dp).wait_recv()
                copy(p, kind + 4, owner, 0, p.rows, to_mate).start()

    def stage4(unit):
        for p in pieces[unit]:
            for kind, owner in ((7, me), (8, left), (9, right), (10, far)):
                copy(p, kind, mate_of(owner), 0, p.rows, to_mate).wait_recv()
            own_copy(p).wait()

    def all_sent(unit):
        for p in pieces[unit]:
            x_off, m_off, _ = geom(p)
            copy(p, 0, me, x_off, p.m + p.c, to_right, True).wait_send()
            copy(p, 1, me, x_off, p.m + p.c, to_left, True).wait_send()
            copy(p, 2, left, m_off, p.m, to_right).wait_send()
            if p.c:
                copy(p, 3, right, p.m, p.c, to_left).wait_send()
            for kind, owner in ((4, left), (5, right), (6, far)):
                copy(p, kind, owner, m_off, p.m, to_dp).wait_send()
            copy(p, 7, me, 0, p.rows, to_mate, True).wait_send()
            for kind, owner in ((8, left), (9, right), (10, far)):
                copy(p, kind, owner, 0, p.rows, to_mate).wait_send()

    pl.semaphore_wait(barrier, n_fsdp)

    def gain_copy(k, owner):
        return pltpu.make_async_remote_copy(
            src_ref=gains_hbm, dst_ref=gains_all.at[owner], send_sem=gain_send.at[k], recv_sem=gain_recv.at[k],
            device_id={'fsdp': (me + k) % n_fsdp}, device_id_type=MESH)

    own_gain = pltpu.make_async_copy(gains_hbm, gains_all.at[me], gain_recv.at[0])
    own_gain.start()
    for k in range(1, n_fsdp):
        gain_copy(k, me).start()
    start_own(0)
    start_own(1)
    own_gain.wait()
    for k in range(1, n_fsdp):
        gain_copy(k, (me + n_fsdp - k) % n_fsdp).wait_recv()

    lane_row = lax.broadcasted_iota(jnp.int32, (1, 128), 1)
    gain_rows = [None] * ((d_model + q_rank + kv_rank) // 128)

    def put(row, value):
        gain_rows[row] = value if gain_rows[row] is None else gain_rows[row] + value

    for owner in range(n_fsdp):
        base_row, local_row = 0, 0
        for total in (d_model, q_rank, kv_rank):
            count = total // n_fsdp
            for r in range(-(-count // 128)):
                size = min(128, count - 128 * r)
                at = owner * count + 128 * r
                row, off = base_row + at // 128, at % 128
                value = gains_all[owner, local_row:local_row + 1, :]
                if off:
                    value = pltpu.roll(value, off, 1)
                    put(row, jnp.where(lane_row >= off, value, 0.0))
                    if off + size > 128:
                        put(row + 1, jnp.where(lane_row < off, value, 0.0))
                else:
                    put(row, value)
                local_row += 1
            base_row += total // 128
    gains = jnp.concatenate(gain_rows, axis=0)
    g_rows = d_model // 128
    q_rows = q_rank // 128
    kv_rows = kv_rank // 128

    def norm_step(blk, carry):
        x_copy(blk).wait()
        row0 = pl.multiple_of(blk * BLOCK, BLOCK)
        for r in range(0, BLOCK, 32):
            xb = a_buf[pl.ds(row0 + r, 32), :].astype(F32)
            inv = lax.rsqrt(jnp.sum(xb * xb, axis=-1, keepdims=True) * (1.0 / d_model) + EPSILON)
            for j in range(g_rows):
                a_buf[pl.ds(row0 + r, 32), j * 128:(j + 1) * 128] = (
                    xb[:, j * 128:(j + 1) * 128] * inv * gains[j:j + 1, :]).astype(BF16)
        return carry

    def tick_a(t):
        stage1(t)
        for unit in AHEAD.get(t, (t + 2,)):
            start_own(unit)

    def lat_step(blk, carry):
        rows = pl.ds(pl.multiple_of(blk * TALL, TALL), TALL)
        u_buf[rows, :] = jnp.dot(a_buf[rows, :], w_dkv[...], preferred_element_type=F32)
        return carry

    def lat_finish(blk):
        rows = pl.ds(pl.multiple_of(blk * BLOCK, BLOCK), BLOCK)
        lat = u_buf[rows, :kv_rank]
        inv = lax.rsqrt(jnp.sum(lat * lat, axis=-1, keepdims=True) * (1.0 / kv_rank) + EPSILON)
        for j in range(kv_rows):
            lat_buf[rows, j * 128:(j + 1) * 128] = (
                lat[:, j * 128:(j + 1) * 128] * inv * gains[g_rows + q_rows + j:g_rows + q_rows + j + 1, :]).astype(BF16)
        pe = jnp.concatenate([u_buf[rows, kv_rank:], jnp.zeros((BLOCK, 128 - rope_dim), F32)], axis=-1)
        cs = jnp.concatenate([cos_r[...]] * (BLOCK // seq_len), axis=0)
        lo = jnp.concatenate([sin_lo[...]] * (BLOCK // seq_len), axis=0)
        hi = jnp.concatenate([sin_hi[...]] * (BLOCK // seq_len), axis=0)
        rot = pe * cs - pltpu.roll(pe, 128 - half, 1) * lo + pltpu.roll(pe, half, 1) * hi
        rot = rot.astype(BF16)
        pe_buf[rows, :] = rot[:, :rope_dim]
        rcomb[rows, :] = rot

    def run(fn, lo, hi):
        lax.fori_loop(lo, hi, fn, 0)

    n_tall = n_tok // TALL
    mid = n_tall // 2
    run(norm_step, 0, 2)
    tick_a(0)
    run(norm_step, 2, 4)
    tick_a(1)
    run(norm_step, 4, 6)
    stage2(0)
    run(norm_step, 6, n_blk)
    tick_a(2)
    stage2(1)
    stage3(0)
    tick_a(3)
    stage4(0)
    stage2(2)
    run(lat_step, 0, 1)
    stage3(1)
    run(lat_step, 1, mid)
    tick_a(4)
    run(lat_step, mid, mid + 1)
    stage2(3)
    stage3(2)
    run(lat_step, mid + 1, n_tall)
    for cp in tab_copies:
        cp.wait()
    def qd_cut(j, lo, hi):
        def qd_step(blk, carry):
            rows = pl.ds(pl.multiple_of(blk * TALL, TALL), TALL)
            qd_buf[rows, j * cut:(j + 1) * cut] = jnp.dot(a_buf[rows, :], w_dq[j], preferred_element_type=F32)
            if j == 0:
                for k in range(TALL // BLOCK):
                    lat_finish(blk * (TALL // BLOCK) + k)
            return carry

        lax.fori_loop(lo, hi, qd_step, 0)

    stage4(1)
    qd_cut(0, 0, mid)
    tick_a(5)
    stage2(4)
    qd_cut(0, mid, n_tall)
    stage3(3)
    stage4(2)
    lat_out = pltpu.make_async_copy(lat_buf, lat_hbm, fin_sem.at[0])
    pe_out = pltpu.make_async_copy(pe_buf, pe_hbm, fin_sem.at[1])
    lat_out.start()
    pe_out.start()

    qd_cut(1, 0, mid)
    tick_a(6)
    stage2(5)
    qd_cut(1, mid, n_tall)
    stage3(4)
    stage4(3)
    qd_cut(2, 0, mid)
    tick_a(7)
    qd_cut(2, mid, n_tall)
    stage2(6)
    stage3(5)

    def cq_step(blk, carry):
        rows = pl.ds(pl.multiple_of(blk * BLOCK, BLOCK), BLOCK)
        qd = qd_buf[rows, :]
        inv = lax.rsqrt(jnp.sum(qd * qd, axis=-1, keepdims=True) * (1.0 / q_rank) + EPSILON)
        for j in range(q_rows):
            cq_buf[rows, j * 128:(j + 1) * 128] = (
                qd[:, j * 128:(j + 1) * 128] * inv * gains[g_rows + j:g_rows + j + 1, :]).astype(BF16)
        return carry

    lax.fori_loop(0, n_blk, cq_step, 0)
    stage4(4)

    n_steps = GROUPS * n_blk

    def out_copy(j):
        return pltpu.make_async_copy(w_out.at[j], wout_hbm.at[:, pl.ds(j * out_cols, out_cols)], fin_sem.at[2 + j])

    first_out = 1 + DQ_CUTS + GROUPS

    def finish_out(unit):
        stage4(unit)
        out_copy(unit - first_out).start()

    plan = [(0, tick_a, 8), (1, stage2, 7), (2, stage3, 6), (4, tick_a, 9), (5, stage2, 8), (5, stage3, 7), (8, stage4, 5), (9, stage3, 8), (9, stage2, 9), (9, tick_a, 10), (13, stage3, 9), (13, tick_a, 11), (14, stage2, 10), (16, stage4, 6), (17, finish_out, 9), (18, stage3, 10), (18, stage2, 11), (18, tick_a, 12), (22, finish_out, 10), (22, stage3, 11), (22, tick_a, 13), (23, stage2, 12), (24, stage4, 7), (26, finish_out, 11), (27, stage3, 12), (27, stage2, 13), (31, finish_out, 12), (31, stage3, 13), (32, stage4, 8), (35, finish_out, 13)]
    schedule = {}
    late = [(fn, unit) for at, fn, unit in plan if at >= n_steps]
    for at, fn, unit in plan:
        schedule.setdefault(at, []).append((fn, unit))
    n_pairs = heads_per_group // 2
    scale = head_q ** -0.5
    c2 = scale * math.log2(math.e)
    mask_val = -1e30 / scale

    def o_copy(g, row0, slot):
        return pltpu.make_async_copy(
            o_blk.at[slot], o_hbm.at[pl.ds(row0, BLOCK), pl.ds(pl.multiple_of(g * heads_per_group * v_dim, 128),
                                                              heads_per_group * v_dim)], o_sem.at[slot])

    def attn_step(step, carry):
        g = step // n_blk
        blk = step % n_blk
        slot = step % 2
        row0 = pl.multiple_of(blk * BLOCK, BLOCK)
        rows = pl.ds(row0, BLOCK)
        for part in range(GROUPS):
            @pl.when(g == part)
            def _():
                for at, todo in schedule.items():
                    if at // n_blk == part:
                        @pl.when(step == at)
                        def _():
                            for fn, unit in todo:
                                fn(unit)

        @pl.when(blk == 0)
        def _():
            for j in range(uq_cols // 128):
                wqt[j * 128:(j + 1) * 128, :] = w_uq[g, :, j * 128:(j + 1) * 128].T
            low = lax.broadcasted_iota(jnp.int32, (kv_rank, 128), 1) < nope
            for j in range(n_pairs):
                even = w_ukv[g, :, (2 * j) * 128:(2 * j + 1) * 128].astype(F32)
                odd = w_ukv[g, :, (2 * j + 1) * 128:(2 * j + 2) * 128].astype(F32)
                wk[:, j * 128:(j + 1) * 128] = jnp.where(low, even, pltpu.roll(odd, nope, 1)).astype(BF16)
                wvt[j * 128:(j + 1) * 128, :] = jnp.where(low, pltpu.roll(even, nope, 1), odd).astype(BF16).T

        @pl.when(step >= 2)
        def _():
            o_copy(0, 0, slot).wait()

        @pl.when(step < n_steps)
        def _():
            qf[...] = nt_dot(wqt[...], cq_buf[rows, :])
            kf[...] = jnp.dot(lat_buf[rows, :], wk[...], preferred_element_type=F32).astype(BF16)
            vt[...] = nt_dot(wvt[...], lat_buf[rows, :]).astype(BF16)

        keep = lax.broadcasted_iota(jnp.int32, (seq_len, 2 * seq_len), 0) <= lax.broadcasted_iota(
            jnp.int32, (seq_len, 2 * seq_len), 1) % seq_len
        ct, st = cos_t[...], sin_t[...]
        rc = rcomb[rows, :]
        zero = jnp.zeros((nope, seq_len), BF16)
        tail = jnp.zeros((128 - rope_dim, 2 * seq_len), BF16)
        @pl.when(step < n_steps)
        def _():
            for pair in range(n_pairs):
                q_nope, q_pe = [], []
                for h in (2 * pair, 2 * pair + 1):
                    q0 = h * head_q
                    v1 = qf[q0 + nope:q0 + nope + half, :]
                    v2 = qf[q0 + nope + half:q0 + head_q, :]
                    q_nope.append(qf[q0:q0 + nope, :].astype(BF16))
                    q_pe.append(jnp.concatenate([(v1 * ct - v2 * st).astype(BF16), (v2 * ct + v1 * st).astype(BF16)], axis=0))
                cols = slice(pair * 128, (pair + 1) * 128)
                for p in range(BLOCK // seq_len):
                    tok = slice(p * seq_len, (p + 1) * seq_len)
                    k_all = jnp.concatenate([kf[tok, cols], rc[tok, :]], axis=1)
                    q_all = jnp.concatenate([
                        jnp.concatenate([q_nope[0][:, tok], zero], axis=1),
                        jnp.concatenate([zero, q_nope[1][:, tok]], axis=1),
                        jnp.concatenate([q_pe[0][:, tok], q_pe[1][:, tok]], axis=1),
                        tail], axis=0)
                    sbuf[2 * pair + p] = jnp.dot(k_all, q_all, preferred_element_type=F32)

        @pl.when(step < n_steps)
        def _():
            for pair in range(n_pairs):
                cols = slice(pair * 128, (pair + 1) * 128)
                for p in range(BLOCK // seq_len):
                    tok = slice(p * seq_len, (p + 1) * seq_len)
                    s_t = sbuf[2 * pair + p]
                    s_t = jnp.where(keep, s_t, mask_val)
                    top = jnp.max(s_t, axis=0, keepdims=True)
                    e_t = jnp.exp2((s_t - top) * c2)
                    tot = jnp.sum(e_t, axis=0, keepdims=True)
                    p_t = (e_t * (1.0 / tot)).astype(BF16)
                    both = jnp.dot(vt[cols, tok], p_t, preferred_element_type=F32)
                    both = jnp.concatenate([both[:v_dim, :seq_len], both[v_dim:, seq_len:]], axis=0)
                    o_blk[slot, tok, cols] = both.astype(BF16).T
        o_copy(g, row0, slot).start()
        return carry

    lax.fori_loop(0, n_steps, attn_step, 0)
    for fn, unit in late:
        fn(unit)

    for slot in range(2):
        o_copy(0, 0, slot).wait()
    lat_out.wait()
    pe_out.wait()
    for unit in range(n_units):
        all_sent(unit)
    for k in range(1, n_fsdp):
        gain_copy(k, me).wait_send()
    for j in range(OUT_CUTS):
        out_copy(j).wait()


def attention_part(x, gains, dq_s, uq_s, dkv_s, ukv_s, out_s, n_fsdp, seq_len, q_rank, kv_rank):
    n_tok, d_model = x.shape
    rope_dim = dkv_s.shape[1] - kv_rank
    v_total = out_s.shape[0] * n_fsdp
    nope_total = ukv_s.shape[1] - v_total
    n_heads = (uq_s.shape[1] - nope_total) // rope_dim
    nope, v_dim = nope_total // n_heads, v_total // n_heads
    hpg = n_heads // GROUPS
    half = rope_dim // 2
    cos_s, sin_s = rope_tables(seq_len, rope_dim)
    pad = np.zeros((seq_len, 128 - rope_dim), np.float32)
    zero = np.zeros((seq_len, half), np.float32)
    tab_r = jnp.asarray(np.stack([np.concatenate(parts, axis=1) for parts in (
        (cos_s, cos_s, pad), (sin_s, zero, pad), (zero, sin_s, pad))]))
    reps = BLOCK // seq_len
    tab_t = jnp.asarray(np.stack([np.concatenate([t.T] * reps, axis=1) for t in (cos_s, sin_s)]))
    dims = (n_fsdp, seq_len, kv_rank, rope_dim, nope, v_dim, hpg)
    n_pieces = 1 + DQ_CUTS + 2 * GROUPS + OUT_CUTS
    any_spec = pl.BlockSpec(memory_space=pl.ANY)
    dma = pltpu.SemaphoreType.DMA
    return pl.pallas_call(
        functools.partial(gather_kernel, dims),
        out_shape=(
            jax.ShapeDtypeStruct((n_tok, v_total), BF16),
            jax.ShapeDtypeStruct((n_tok, kv_rank), BF16),
            jax.ShapeDtypeStruct((n_tok, rope_dim), BF16),
            jax.ShapeDtypeStruct((v_total, d_model), BF16),
        ),
        in_specs=[any_spec] * 9,
        out_specs=(any_spec,) * 4,
        scratch_shapes=[
            pltpu.VMEM(tab_r.shape, F32),
            pltpu.VMEM(tab_t.shape, F32),
            pltpu.VMEM((n_fsdp,) + gains.shape, F32),
            pltpu.VMEM((dkv_s.shape[0] * n_fsdp, dkv_s.shape[1]), BF16),
            pltpu.VMEM((DQ_CUTS, d_model, q_rank // DQ_CUTS), BF16),
            pltpu.VMEM((GROUPS, q_rank, uq_s.shape[1] // GROUPS), BF16),
            pltpu.VMEM((GROUPS, kv_rank, ukv_s.shape[1] // GROUPS), BF16),
            pltpu.VMEM((OUT_CUTS, v_total, d_model // OUT_CUTS), BF16),
            pltpu.VMEM((n_tok, d_model), BF16),
            pltpu.VMEM((n_tok, q_rank), F32),
            pltpu.VMEM((n_tok, q_rank), BF16),
            pltpu.VMEM((n_tok, kv_rank), BF16),
            pltpu.VMEM((n_tok, rope_dim), BF16),
            pltpu.VMEM((n_tok, 128), BF16),
            pltpu.VMEM((n_tok, dkv_s.shape[1]), F32),
            pltpu.VMEM((hpg * (nope + rope_dim), q_rank), BF16),
            pltpu.VMEM((kv_rank, hpg * nope), BF16),
            pltpu.VMEM((hpg * v_dim, kv_rank), BF16),
            pltpu.VMEM((hpg * (nope + rope_dim), BLOCK), F32),
            pltpu.VMEM((BLOCK, hpg * nope), BF16),
            pltpu.VMEM((hpg * v_dim, BLOCK), BF16),
            pltpu.VMEM((hpg, 128, 256), F32),
            pltpu.VMEM((2, BLOCK, hpg * v_dim), BF16),
            dma((n_pieces, N_KINDS)),
            dma((n_pieces, N_KINDS)),
            dma((n_pieces,)),
            dma((n_fsdp,)),
            dma((n_fsdp,)),
            dma((n_tok // BLOCK,)),
            dma((2,)),
            dma((2 + OUT_CUTS,)),
            dma((2,)),
        ],
        compiler_params=pltpu.CompilerParams(
            collective_id=0, has_side_effects=True, vmem_limit_bytes=67043328),
        name='latent_attention',
    )(x, gains, dq_s, uq_s, dkv_s, ukv_s, out_s, tab_r, tab_t)


def solution(mesh):
    batch_spec = P(('dp', 'fsdp'))
    row_spec = P('fsdp')
    mat_spec = P('fsdp', None)
    n_fsdp = mesh.shape['fsdp']

    def run_block(tokens, gain_in, w_dq, gain_q, w_uq, w_dkv, gain_kv, w_ukv, w_out):
        seq_len = tokens.shape[1]

        def local_block(tok_blk, g_in, dq_s, g_q, uq_s, dkv_s, g_kv, ukv_s, out_s):
            n_prompts, _, d_model = tok_blk.shape
            parts = [jnp.pad(g.astype(F32), (0, -g.shape[0] % 128)) for g in (g_in, g_q, g_kv)]
            flat = jnp.concatenate(parts)
            gains = jnp.pad(flat, (0, -flat.shape[0] % 1024)).reshape(-1, 128)
            x = tok_blk.reshape(n_prompts * seq_len, d_model)
            attn_out, latent, k_pe, w_out_all = attention_part(
                x, gains, dq_s, uq_s, dkv_s, ukv_s, out_s, n_fsdp, seq_len, g_q.shape[0] * n_fsdp,
                g_kv.shape[0] * n_fsdp)
            proj = jnp.dot(attn_out, w_out_all, preferred_element_type=F32)
            y = (x.astype(F32) + proj).astype(BF16)
            return (y.reshape(tok_blk.shape), latent.reshape(n_prompts, seq_len, -1),
                    k_pe.reshape(n_prompts, seq_len, -1))

        mapped = jax.shard_map(
            local_block,
            mesh=mesh,
            in_specs=(batch_spec, row_spec, mat_spec, row_spec, mat_spec, mat_spec, row_spec, mat_spec, mat_spec),
            out_specs=(batch_spec, batch_spec, batch_spec),
            check_vma=False,
        )
        return mapped(tokens, gain_in, w_dq, gain_q, w_uq, w_dkv, gain_kv, w_ukv, w_out)

    return run_block
```
